32 devices in a mesh: mpo: 4 (over y, x), sec: 8 (over z, core).
Axes of the slice: x: 2, y: 2, z: 4, core: 2. Of those that a mesh axis runs over, the one named last changes fastest.
Arguments:
- wavefunction: bfloat16 [8, 256, 256], P('sec'), may hold values from -6 to 6
- left_dims: int32 [8], P('sec'), may hold values from 64 to 256
- right_dims: int32 [8], P('sec'), may hold values from 64 to 256
- left_environment_block: bfloat16 [1280, 256, 256], P(('mpo', 'sec')), may hold values from -0.375 to 0.375
- right_env: bfloat16 [1280, 256, 256], P(('mpo', 'sec')), may hold values from -0.03125 to 0.03125
- task_out: int32 [1280], P(('mpo', 'sec')), may hold values from 0 to 7
- task_in: int32 [1280], P(('mpo', 'sec')), may hold values from 0 to 7
Outputs:
- applied: bfloat16 [8, 256, 256], P('sec', 'mpo')
The draws below stay inside these ranges and needn't reach their ends.
All inputs are finite; a program needn't handle non-finite values.
Results may differ from the reference program's by a relative error of at most 0.0078.
Values may be sent and summed in bfloat16 or wider, within the bound.
No kernel may reach another device: no remote copies, remote signals or barrier semaphores. Data moves between devices by JAX's collectives and lax.ppermute only.
A program may use at most 128 MiB of HBM per device.

```python
import math
import jax
import jax.numpy as jnp
import numpy as np
from jax import lax

BLK = 256
TASKS_DEV = 40
S = 8
TASKS = 1280


def place_ends(array, own_key, least, high):
    longest = array.shape.index(max(array.shape))
    spots = []
    for shift in (0, 1):
        where = [jax.random.randint(jax.random.fold_in(own_key, axis), (), 0, length) for axis, length in enumerate(array.shape)]
        where[longest] = (where[longest] + shift) % array.shape[longest]
        spots.append(tuple(where))
    return array.at[spots[0]].set(least).at[spots[1]].set(high)


def levels(stream_key, extent, split, low, high):
    level, own = 1.0, jax.random.fold_in(stream_key, 6)
    for dim, blocks in split:
        draws = jnp.exp(jax.random.uniform(jax.random.fold_in(own, dim), (blocks,), jnp.float32, low / len(split), high / len(split)))
        level = level * jnp.repeat(draws, extent[dim] // blocks).reshape([-1 if axis == dim else 1 for axis in range(len(extent))])
    return level


def cumulative_ranks(count, lean):
    weights = [(1 << 20) // math.isqrt(grade ** lean) + 1 for grade in range(1, count + 1)]
    width = 1 + sum(weights) // (1 << 30)
    return np.cumsum(np.array([max(1, weight // width) for weight in weights]))


def skewed_ids(own_key, dims, number_of, skew):
    table = cumulative_ranks(number_of, skew)
    ticket = jax.random.randint(jax.random.fold_in(own_key, 1), dims, 0, int(table[number_of - 1]))
    grade = jnp.searchsorted(jnp.asarray(table, jnp.int32), ticket, side="right")
    return jax.random.permutation(jax.random.fold_in(own_key, 2), number_of)[grade].astype(jnp.int32)


def scatter_about(stream_key, shape, deviation, limit, cuts=(), dtype=jnp.bfloat16):
    factor_of = levels(stream_key, shape, cuts, -0.22, 0.18) if cuts else 1.0
    drawn = jax.random.normal(stream_key, shape, jnp.float32) * deviation * factor_of
    return jnp.minimum(jnp.maximum(drawn, -limit), limit).astype(dtype)


def setup_inputs(seed: int = 0) -> dict:
    splits = jax.random.split(jax.random.key(seed), 8)
    return {
        "wavefunction": scatter_about(splits[0], (S, BLK, BLK), 1.0, 6.0, ((0, 8),)),
        "left_dims": place_ends(jax.random.randint(splits[1], (S,), BLK // 4, BLK + 1), jax.random.fold_in(splits[1], 1), BLK // 4, BLK).astype(jnp.int32),
        "right_dims": place_ends(jax.random.randint(splits[2], (S,), BLK // 4, BLK + 1), jax.random.fold_in(splits[2], 1), BLK // 4, BLK).astype(jnp.int32),
        "left_environment_block": scatter_about(splits[3], (TASKS, BLK, BLK), BLK ** -0.5, 0.375, ((0, 32),)),
        "right_env": scatter_about(splits[4], (TASKS, BLK, BLK), (BLK * TASKS // S) ** -0.5, 0.03125, ((0, 32),)),
        "task_out": place_ends(skewed_ids(splits[5], (TASKS,), S, 1), jax.random.fold_in(splits[5], 3), 0, S - 1).astype(jnp.int32),
        "task_in": place_ends(jax.random.randint(splits[6], (TASKS,), 0, S), jax.random.fold_in(splits[6], 1), 0, S - 1).astype(jnp.int32),
    }


def reference(wavefunction, left_dims, right_dims, left_environment_block, right_env, task_out, task_in):
    row_ids = lax.broadcasted_iota(jnp.int32, wavefunction.shape, 1)
    col_ids = lax.broadcasted_iota(jnp.int32, wavefunction.shape, 2)
    live_cells = (row_ids < left_dims[:, None, None]) & (col_ids < right_dims[:, None, None])
    masked = jnp.where(live_cells, wavefunction, jnp.zeros_like(wavefunction))
    rounds = TASKS // TASKS_DEV
    left_parts = left_environment_block.reshape(rounds, TASKS_DEV, BLK, BLK)
    right_parts = right_env.reshape(rounds, TASKS_DEV, BLK, BLK)
    out_parts = task_out.astype(jnp.int32).reshape(rounds, TASKS_DEV)
    input_pieces = task_in.astype(jnp.int32).reshape(rounds, TASKS_DEV)

    def accumulate(summed, pieces):
        left_piece, right_piece, out_ids, in_ids = pieces
        picked_tasks = jnp.take(masked, in_ids, axis=0).astype(jnp.float32)
        middle_tensor = jnp.einsum("xvz,xzy->xvy", left_piece.astype(jnp.float32), picked_tasks).astype(jnp.bfloat16)
        task_product = jnp.einsum("hzk,hlk->hzl", middle_tensor.astype(jnp.float32), right_piece.astype(jnp.float32))
        return summed + jax.ops.segment_sum(task_product, out_ids, num_segments=S), None

    summed, _ = lax.scan(accumulate, jnp.zeros((S, BLK, BLK), jnp.float32), (left_parts, right_parts, out_parts, input_pieces))
    return jnp.where(live_cells, summed, jnp.zeros_like(summed)).astype(jnp.bfloat16)
```

```python
import functools

import jax
import jax.numpy as jnp
from jax import lax
from jax.experimental import pallas as pl
from jax.experimental.pallas import tpu as pltpu
from jax.sharding import PartitionSpec as P

CORES = 2
VMEM = pltpu.VMEM
SMEM = pltpu.SMEM


def shift(value, axis, distance, stride=1):
    size = lax.axis_size(axis)
    ring = size // stride
    pairs = [(i, (i // stride + distance) % ring * stride + i % stride) for i in range(size)]
    return lax.ppermute(value, axis, pairs)


def swap(value):
    return lax.ppermute(value, "sec", [(i, i ^ 1) for i in range(lax.axis_size("sec"))])


def contract(groups, depth, chunk, *refs):
    task_in, task_out, own, near = refs[:4]
    mine, theirs = refs[4 : 4 + groups], refs[4 + groups : 4 + 2 * groups]
    left, right, send, keep, blocks, acc, left_buf, right_buf, sems = refs[4 + 2 * groups :]
    tasks = left.shape[0]
    size = own.shape[1]
    quarter = size // groups
    chunks = tasks // chunk

    def fetch(n, which):
        source, target = ((left, left_buf), (right, right_buf))[which]
        span = pl.ds(n * chunk, chunk)
        return pltpu.make_async_copy(source.at[span], target.at[span], sems.at[which, n])

    for n in range(chunks):
        fetch(n, 0).start()
        fetch(n, 1).start()

    sec = lax.axis_index("sec")
    layer, core = sec // CORES, sec % CORES
    group = lax.axis_index("mpo")
    blocks[sec] = own[0]
    blocks[sec + 1 - 2 * core] = near[0]

    def place(k, _):
        base = lax.rem(layer + depth - 1 - k, depth) * CORES
        for j in range(groups):
            rows = pl.ds(pl.multiple_of(lax.rem(group + groups - j, groups) * quarter, quarter), quarter)
            blocks[base + core, rows] = mine[j][k]
            blocks[base + 1 - core, rows] = theirs[j][k]
        return 0

    lax.fori_loop(0, depth - 1, place, 0)
    acc[...] = jnp.zeros_like(acc)

    def step(n, _):
        fetch(n, 0).wait()
        fetch(n, 1).wait()
        for u in range(chunk):
            t = n * chunk + u
            middle = jnp.dot(
                left_buf[t], blocks[task_in[t]], preferred_element_type=jnp.float32
            ).astype(jnp.bfloat16)
            acc[task_out[t]] += lax.dot_general(
                middle, right_buf[t], (((1,), (1,)), ((), ())), preferred_element_type=jnp.float32
            )
        return 0

    lax.fori_loop(0, chunks, step, 0)

    def put(k, _):
        base = lax.rem(layer + k, depth) * CORES
        for j in range(groups):
            rows = pl.ds(pl.multiple_of(lax.rem(group + j, groups) * quarter, quarter), quarter)
            keep[j, k] = acc[base + core, rows]
            send[j, k] = acc[base + 1 - core, rows].astype(send.dtype)
        return 0

    lax.fori_loop(0, depth, put, 0)


def merge_cores(groups, keep, got, total, *sends):
    total[...] = keep[0] + got[0].astype(jnp.float32)
    for j in range(1, groups):
        sends[j - 1][...] = (keep[j] + got[j].astype(jnp.float32)).astype(jnp.bfloat16)


def merge_groups(groups, depth, *refs):
    keep, gots = refs[0], refs[1:groups]
    total, sends = refs[groups], refs[groups + 1 :]
    for k in range(depth):
        value = keep[k]
        for got in gots:
            value += got[k].astype(jnp.float32)
        if k == 0:
            total[...] = value
        else:
            sends[k - 1][...] = value.astype(jnp.bfloat16)


def whole_in_vmem(count):
    return [pl.BlockSpec(memory_space=VMEM)] * count


def on_device(
    wavefunction, left_dims, right_dims, left_environment_block, right_env, task_out, task_in
):
    rows, cols = wavefunction.shape[1:]
    groups = lax.axis_size("mpo")
    sectors = lax.axis_size("sec")
    depth = sectors // CORES
    quarter = rows // groups
    tasks = task_out.shape[0]
    group = lax.axis_index("mpo")
    bf16, f32 = jnp.bfloat16, jnp.float32

    def live(shape, first_row):
        row_ids = lax.broadcasted_iota(jnp.int32, shape, 1) + first_row
        col_ids = lax.broadcasted_iota(jnp.int32, shape, 2)
        return (row_ids < left_dims[:, None, None]) & (col_ids < right_dims[:, None, None])

    part = lax.dynamic_slice_in_dim(wavefunction, group * quarter, quarter, axis=1)
    part = jnp.where(live(part.shape, group * quarter), part, jnp.zeros_like(part))
    layers = [shift(part, "sec", k, CORES) for k in range(1, depth)]
    own = jnp.where(live(wavefunction.shape, 0), wavefunction, jnp.zeros_like(wavefunction))
    near = swap(own)
    mine = [jnp.concatenate(layers, axis=0)]
    mine += [shift(mine[0], "mpo", j) for j in range(1, groups)]
    theirs = [swap(piece) for piece in mine]

    chunk = 4 if tasks % 4 == 0 else 1
    send, keep = pl.pallas_call(
        functools.partial(contract, groups, depth, chunk),
        out_shape=(
            jax.ShapeDtypeStruct((groups, depth, quarter, cols), bf16),
            jax.ShapeDtypeStruct((groups, depth, quarter, cols), f32),
        ),
        in_specs=[pl.BlockSpec(memory_space=SMEM)] * 2
        + whole_in_vmem(2 + 2 * groups)
        + [pl.BlockSpec(memory_space=pl.ANY)] * 2,
        out_specs=tuple(whole_in_vmem(2)),
        scratch_shapes=[
            VMEM((sectors, rows, cols), bf16),
            VMEM((sectors, rows, cols), f32),
            VMEM(left_environment_block.shape, bf16),
            VMEM(right_env.shape, bf16),
            pltpu.SemaphoreType.DMA((2, tasks // chunk)),
        ],
        cost_estimate=pl.CostEstimate(
            flops=4 * tasks * rows * cols * rows,
            bytes_accessed=4 * tasks * rows * cols,
            transcendentals=0,
        ),
        name="contract",
    )(task_in, task_out, own, near, *mine, *theirs, left_environment_block, right_env)

    got = swap(send)
    total, *sends = pl.pallas_call(
        functools.partial(merge_cores, groups),
        out_shape=(jax.ShapeDtypeStruct((depth, quarter, cols), f32),)
        + (jax.ShapeDtypeStruct((depth, quarter, cols), bf16),) * (groups - 1),
        in_specs=whole_in_vmem(2),
        out_specs=tuple(whole_in_vmem(groups)),
        name="merge_cores",
    )(keep, got)
    gots = [shift(piece, "mpo", j + 1) for j, piece in enumerate(sends)]
    total, *sends = pl.pallas_call(
        functools.partial(merge_groups, groups, depth),
        out_shape=(jax.ShapeDtypeStruct((quarter, cols), f32),)
        + (jax.ShapeDtypeStruct((quarter, cols), bf16),) * (depth - 1),
        in_specs=whole_in_vmem(groups),
        out_specs=tuple(whole_in_vmem(depth)),
        name="merge_groups",
    )(total, *gots)
    for k, piece in enumerate(sends):
        total = total + shift(piece, "sec", k + 1, CORES).astype(f32)
    total = total[None]
    return jnp.where(live(total.shape, group * quarter), total, jnp.zeros_like(total)).astype(bf16)


def solution(mesh):
    return jax.shard_map(
        on_device,
        mesh=mesh,
        in_specs=(
            P("sec", None, None),
            P("sec"),
            P("sec"),
            P(("mpo", "sec"), None, None),
            P(("mpo", "sec"), None, None),
            P(("mpo", "sec")),
            P(("mpo", "sec")),
        ),
        out_specs=P("sec", "mpo", None),
        check_vma=False,
    )
```

```python
import functools
import math

import jax
import jax.numpy as jnp
from jax import lax
from jax.experimental import pallas as pl
from jax.experimental.pallas import tpu as pltpu
from jax.sharding import PartitionSpec as P

CORES = 2
UNROLL = 4
VMEM_BYTES = 67043328
SLACK = 1 << 20
VMEM = pltpu.VMEM
SMEM = pltpu.SMEM
BF16 = jnp.bfloat16
F32 = jnp.float32


def shift(value, axis, distance, stride=1):
    size = lax.axis_size(axis)
    ring = size // stride
    pairs = [(i, (i // stride + distance) % ring * stride + i % stride) for i in range(size)]
    return lax.ppermute(value, axis, pairs)


def swap(value):
    return lax.ppermute(value, "sec", [(i, i ^ 1) for i in range(lax.axis_size("sec"))])


def array(shape, dtype):
    return jax.ShapeDtypeStruct(shape, dtype)


def grant(scratch, *operands):
    mine, others = (sum(math.prod(a.shape) * a.dtype.itemsize for a in group) for group in (scratch, operands))
    return mine + SLACK if 2 * (mine + others) < VMEM_BYTES else min(mine + others + 2 * SLACK, VMEM_BYTES)


def call(kernel, name, out_shape, operands, scratch=(), scalars=0, cost=None, aliases=None, streamed=()):
    one = not isinstance(out_shape, tuple)
    outs = (out_shape,) if one else out_shape
    specs = [pl.BlockSpec(memory_space=SMEM)] * scalars
    specs += [pl.BlockSpec(memory_space=VMEM)] * (len(operands) - scalars)
    for n in streamed:
        specs[n] = pl.BlockSpec(memory_space=pl.ANY)
    results = pl.pallas_call(
        kernel,
        out_shape=outs,
        in_specs=specs,
        out_specs=(pl.BlockSpec(memory_space=VMEM),) * len(outs),
        scratch_shapes=scratch,
        cost_estimate=cost,
        input_output_aliases=aliases or {},
        compiler_params=pltpu.CompilerParams(
            vmem_limit_bytes=grant(
                [s for s in scratch if getattr(s, "memory_space", None) == VMEM], *outs, *operands[scalars:]
            )
        ),
        name=name,
    )(*operands)
    return results[0] if one else results


def clear(acc):
    acc[...] = jnp.zeros_like(acc)


def products(distances, late, task_in, task_out, blocks, left, right, acc, order, middle, *stage):
    tasks = left.shape[0]
    depth = acc.shape[0] // CORES
    layer = lax.axis_index("sec") // CORES
    others = [d for d in range(depth) if d not in distances]
    shorter = min(distances, others, key=len)
    layers = [lax.rem(layer + depth - d, depth) for d in shorter]
    count = jnp.int32(0)
    for t in range(tasks):
        source = lax.div(task_in[t], CORES)
        listed = functools.reduce(jnp.logical_or, [source == it for it in layers])
        order[count] = t
        count += jnp.where(listed, *((1, 0) if late == (shorter is others) else (0, 1)))
    for u in range(2 * UNROLL):
        order[count + u] = tasks

    def task(slot):
        t = order[slot]
        return jnp.where(t < tasks, t, 0), t < tasks

    def fetch(which, t, u):
        source = (left, right)[which]
        if not stage:
            return source[t]
        target, sems = stage
        copy = pltpu.make_async_copy(source.at[t], target.at[which, u], sems.at[which, u])
        copy.start()
        copy.wait()
        return target[which, u]

    def first(n):
        for u in range(UNROLL):
            t, _ = task(n * UNROLL + u)
            product = jnp.dot(fetch(0, t, u), blocks[task_in[t]], preferred_element_type=F32)
            middle[u] = product.astype(BF16)

    def second(n):
        for u in range(UNROLL):
            t, real = task(n * UNROLL + u)
            target = jnp.where(real, task_out[t], acc.shape[0] - 1)
            acc[target] += lax.dot_general(
                middle[u], fetch(1, t, u), (((1,), (1,)), ((), ())), preferred_element_type=F32
            )

    def step(n, _):
        second(n)
        first(n + 1)
        return 0

    first(0)
    lax.fori_loop(0, (count + UNROLL - 1) // UNROLL, step, 0)


def place(blocks, distances, found):
    depth = blocks.shape[0] // CORES
    sec = lax.axis_index("sec")
    layer, core = sec // CORES, sec % CORES
    parts = len(found) // max(1, CORES * len(distances))
    found = iter(found)
    for distance in distances:
        base = lax.rem(layer + depth - distance, depth) * CORES
        for sector in (base + core, base + 1 - core):
            for part in range(parts):
                block = next(found)
                size = block.shape[1]
                blocks[sector, part * size : (part + 1) * size] = block[0]


def contract_early(sources, near, count, task_in, task_out, *refs):
    found, (left, right, _, acc, blocks), rest = refs[:count], refs[count : count + 5], refs[count + 5 :]
    place(blocks, sources, found)
    products(near, False, task_in, task_out, blocks, left, right, acc, *rest)


def contract_late(sources, near, count, task_in, task_out, *refs):
    found, (left, right, _, acc), refs = refs[:count], refs[count : count + 4], refs[count + 4 :]
    groups = lax.axis_size("mpo")
    sends, keeps, (blocks, *rest) = refs[:groups], refs[groups : 2 * groups], refs[2 * groups :]
    if sources:
        place(blocks, sources, found)
        products(near, True, task_in, task_out, blocks, left, right, acc, *rest)
    depth, quarter = sends[0].shape[:2]
    sec = lax.axis_index("sec")
    layer, core = sec // CORES, sec % CORES
    group = lax.axis_index("mpo")

    def put(k, _):
        base = lax.rem(layer + k, depth) * CORES
        for j in range(groups):
            rows = pl.ds(pl.multiple_of(lax.rem(group + j, groups) * quarter, quarter), quarter)
            keeps[j][k] = acc[base + core, rows]
            sends[j][k] = acc[base + 1 - core, rows].astype(BF16)
        return 0

    lax.fori_loop(0, depth, put, 0)


def merge_cores(keep, got, send):
    send[...] = (keep[...] + got[...].astype(F32)).astype(BF16)


def merge_groups(depth, *refs):
    terms, (total, *sends) = refs[:-depth], refs[-depth:]
    for k in range(depth):
        value = functools.reduce(jnp.add, [term[k].astype(F32) for term in terms])
        if k == 0:
            total[...] = value
        else:
            sends[k - 1][...] = value.astype(BF16)


def on_device(
    wavefunction, left_dims, right_dims, left_environment_block, right_env, task_out, task_in
):
    rows, cols = wavefunction.shape[1:]
    groups = lax.axis_size("mpo")
    sectors = lax.axis_size("sec")
    depth = sectors // CORES
    quarter = rows // groups
    tasks = task_out.shape[0]
    group = lax.axis_index("mpo")

    def live(shape, first_row):
        row_ids = lax.broadcasted_iota(jnp.int32, shape, 1) + first_row
        col_ids = lax.broadcasted_iota(jnp.int32, shape, 2)
        return (row_ids < left_dims[:, None, None]) & (col_ids < right_dims[:, None, None])

    own = jnp.where(live(wavefunction.shape, 0), wavefunction, jnp.zeros_like(wavefunction))
    near = sorted({0, 1 % depth, depth - 1})
    far = [d for d in range(depth) if d not in near]
    mine = {d: [shift(own, "sec", d, CORES) if d else own] for d in near}
    half = rows // 2
    for d in far:
        if far == [2]:
            up, down = mine[1][0][:, :half], mine[3][0][:, half:]
            mine[d] = [shift(up, "sec", 1, CORES), shift(down, "sec", 3, CORES)]
        else:
            mine[d] = [shift(own, "sec", d, CORES)]
    found = {d: [*blocks, *(swap(block) for block in blocks)] for d, blocks in mine.items()}

    work = (left_environment_block, right_env)
    cost = pl.CostEstimate(
        flops=4 * tasks * rows * cols * rows, bytes_accessed=4 * tasks * rows * cols, transcendentals=0
    )
    slow = pl.CostEstimate(flops=4 * cost.flops, bytes_accessed=4 * cost.bytes_accessed, transcendentals=0)
    sums = array((sectors + 1, rows, cols), F32)
    acc = call(clear, "clear", sums, (), cost=slow)
    scratch = (
        VMEM((sectors, rows, cols), BF16),
        SMEM((tasks + 2 * UNROLL,), jnp.int32),
        VMEM((UNROLL, rows, cols), BF16),
    )
    streamed = 16 * sums.size > VMEM_BYTES
    if streamed:
        scratch += (VMEM((2, UNROLL, rows, cols), BF16), pltpu.SemaphoreType.DMA((2, UNROLL)))

    def contract(kernel, sources, outs, **options):
        blocks = [b for d in sources for b in found[d]]
        operands = (task_in, task_out, *blocks, *work, acc)
        last = len(operands) - 1
        return call(
            functools.partial(kernel, sources, near, len(blocks)),
            kernel.__name__,
            outs,
            operands,
            scratch,
            scalars=2,
            aliases={last: 0},
            streamed=(last - 2, last - 1) if streamed else (),
            **options,
        )

    acc = contract(contract_early, near, sums, cost=cost)
    piece = (depth, quarter, cols)
    late_outs = (sums, *(array(piece, BF16),) * groups, *(array(piece, F32),) * groups)
    _, *pieces = contract(contract_late, far, late_outs)
    sends, keeps = pieces[:groups], pieces[groups:]

    gots = {}
    for j in [*range(1, groups), 0]:
        got = swap(sends[j])
        if j:
            gots[j] = shift(call(merge_cores, "merge_cores", array(piece, BF16), (keeps[j], got)), "mpo", j)
        else:
            gots[j] = got
    total, *sends = call(
        functools.partial(merge_groups, depth),
        "merge_groups",
        (array(piece[1:], F32), *(array(piece[1:], BF16),) * (depth - 1)),
        (keeps[0], *(gots[j] for j in range(groups))),
    )
    for k, sent in enumerate(sends):
        total = total + shift(sent, "sec", k + 1, CORES).astype(F32)
    total = total[None]
    return jnp.where(live(total.shape, group * quarter), total, jnp.zeros_like(total)).astype(BF16)


def solution(mesh):
    return jax.shard_map(
        on_device,
        mesh=mesh,
        in_specs=(
            P("sec", None, None),
            P("sec"),
            P("sec"),
            P(("mpo", "sec"), None, None),
            P(("mpo", "sec"), None, None),
            P(("mpo", "sec")),
            P(("mpo", "sec")),
        ),
        out_specs=P("sec", "mpo", None),
        check_vma=False,
    )
```

```python
import functools
import math

import jax
import jax.numpy as jnp
from jax import lax
from jax.experimental import pallas as pl
from jax.experimental.pallas import tpu as pltpu
from jax.sharding import PartitionSpec as P


CORES = 2
UNROLL = 20
DIRECT = (0, 1)
VMEM_BYTES = 67043328
SLACK = 1 << 20
VMEM = pltpu.VMEM
SMEM = pltpu.SMEM
BF16 = jnp.bfloat16
F32 = jnp.float32


def partner(layer, k, depth, back=False):
    if depth & (depth - 1) == 0:
        return layer ^ k
    return lax.rem(layer + (depth - k if back else k), depth) if isinstance(layer, jax.Array) else (layer + k) % depth


def send(value, axis, target):
    return lax.ppermute(value, axis, [(i, target(i)) for i in range(lax.axis_size(axis))])


def along_z(value, k, rule=partner):
    depth = lax.axis_size("sec") // CORES
    return send(value, "sec", lambda i: rule(i // CORES, k, depth) * CORES + i % CORES)


def round_z(layer, k, depth):
    return lax.rem(layer + k, depth) if isinstance(k, jax.Array) else (layer + k) % depth


def along_mpo(value, j):
    groups = lax.axis_size("mpo")
    return send(value, "mpo", lambda i: (i + j) % groups)


def swap(value):
    return send(value, "sec", lambda i: i ^ 1)


def array(shape, dtype):
    return jax.ShapeDtypeStruct(shape, dtype)


def grant(scratch, *operands):
    mine, others = (sum(math.prod(a.shape) * a.dtype.itemsize for a in group) for group in (scratch, operands))
    return mine + SLACK if 2 * (mine + others) < VMEM_BYTES else min(mine + others + 2 * SLACK, VMEM_BYTES)


def call(kernel, out_shape, operands, scratch=(), scalars=0, cost=None, aliases=None, streamed=()):
    one = not isinstance(out_shape, tuple)
    outs = (out_shape,) if one else out_shape
    specs = [pl.BlockSpec(memory_space=SMEM)] * scalars
    specs += [pl.BlockSpec(memory_space=VMEM)] * (len(operands) - scalars)
    for n in streamed:
        specs[n] = pl.BlockSpec(memory_space=pl.ANY)
    run = pl.pallas_call(
        kernel,
        out_shape=outs,
        in_specs=specs,
        out_specs=(pl.BlockSpec(memory_space=VMEM),) * len(outs),
        scratch_shapes=scratch,
        cost_estimate=cost,
        input_output_aliases=aliases or {},
        compiler_params=pltpu.CompilerParams(
            vmem_limit_bytes=grant(
                [s for s in scratch if getattr(s, "memory_space", None) == VMEM], *outs, *operands[scalars:]
            )
        ),
    )
    results = run(*operands)
    return results[0] if one else results


def clear(acc):
    acc[...] = jnp.zeros_like(acc)


def take_rows(own, part):
    quarter = part.shape[1]
    part[...] = own[:, pl.ds(pl.multiple_of(lax.axis_index("mpo") * quarter, quarter), quarter)]


def products(task_in, task_out, blocks, left, right, acc, *stage):
    tasks = left.shape[0]
    limit = stage[0].shape[1] if stage else UNROLL
    unroll = max(n for n in range(1, limit + 1) if tasks % n == 0)

    def fetch(which, t, u):
        source = (left, right)[which]
        if not stage:
            return source[t]
        target, sems = stage
        copy = pltpu.make_async_copy(source.at[t], target.at[which, u], sems.at[which, u])
        copy.start()
        copy.wait()
        return target[which, u]

    def step(n, _):
        for u in range(unroll):
            t = n * unroll + u
            middle = jnp.dot(fetch(0, t, u), blocks[task_in[t]], preferred_element_type=F32).astype(BF16)
            acc[task_out[t]] += lax.dot_general(
                middle, fetch(1, t, u), (((1,), (1,)), ((), ())), preferred_element_type=F32
            )
        return 0

    lax.fori_loop(0, tasks // unroll, step, 0)


def contract(task_in, task_out, *refs):
    groups = lax.axis_size("mpo")
    direct, refs = refs[: CORES * len(DIRECT)], refs[CORES * len(DIRECT) :]
    spread, (left, right, _, acc), refs = refs[: CORES * groups], refs[CORES * groups :][:4], refs[CORES * groups + 4 :]
    sends, keeps, (blocks, *stage) = refs[:groups], refs[groups : 2 * groups], refs[2 * groups :]
    depth, quarter = sends[0].shape[:2]
    sec = lax.axis_index("sec")
    layer, core = sec // CORES, sec % CORES
    group = lax.axis_index("mpo")
    for n, k in enumerate(DIRECT):
        base = partner(layer, k, depth, back=True) * CORES
        blocks[base + core] = direct[CORES * n][0]
        blocks[base + 1 - core] = direct[CORES * n + 1][0]
    for n in range(spread[0].shape[0]):
        base = partner(layer, len(DIRECT) + n, depth, back=True) * CORES
        for j in range(groups):
            start = lax.rem(group + groups - j, groups) * quarter
            rows = pl.ds(pl.multiple_of(start, quarter), quarter)
            blocks[base + core, rows] = spread[CORES * j][n]
            blocks[base + 1 - core, rows] = spread[CORES * j + 1][n]
    products(task_in, task_out, blocks, left, right, acc, *stage)

    def put(k, _):
        base = round_z(layer, k, depth) * CORES
        for j in range(groups):
            rows = pl.ds(pl.multiple_of(lax.rem(group + j, groups) * quarter, quarter), quarter)
            keeps[j][k] = acc[base + core, rows]
            sends[j][k] = acc[base + 1 - core, rows].astype(BF16)
        return 0

    lax.fori_loop(0, depth, put, 0)


def merge_cores(keep, got, away, here):
    value = keep[...] + got[...].astype(F32)
    here[...] = value[:1].astype(BF16)
    away[...] = value[1:].astype(BF16)


def merge_away(depth, *refs):
    terms, sends = refs[: 1 - depth], refs[1 - depth :]
    for k in range(1, depth):
        values = [term[k + term.shape[0] - depth].astype(F32) for term in terms]
        sends[k - 1][...] = functools.reduce(jnp.add, values).astype(BF16)


def merge_here(*refs):
    *terms, total = refs
    total[...] = functools.reduce(jnp.add, [term[0].astype(F32) for term in terms])


def device_step(
    wavefunction, left_dims, right_dims, left_environment_block, right_env, task_out, task_in
):
    rows, cols = wavefunction.shape[1:]
    groups = lax.axis_size("mpo")
    sectors = lax.axis_size("sec")
    depth = sectors // CORES
    quarter = rows // groups
    tasks = task_out.shape[0]
    group = lax.axis_index("mpo")

    def live(shape, first_row):
        row_ids = lax.broadcasted_iota(jnp.int32, shape, 1) + first_row
        col_ids = lax.broadcasted_iota(jnp.int32, shape, 2)
        return (row_ids < left_dims[:, None, None]) & (col_ids < right_dims[:, None, None])

    own = jnp.where(live(wavefunction.shape, 0), wavefunction, jnp.zeros_like(wavefunction))
    part = call(take_rows, array((1, quarter, cols), BF16), (own,))
    far = [along_z(part, k) for k in range(len(DIRECT), depth)]
    near = [own, *(along_z(own, k) for k in DIRECT[1:])]
    pieces = [jnp.concatenate(far, axis=0)]
    pieces += [along_mpo(pieces[0], j) for j in range(1, groups)]
    blocks = [b for block in near for b in (block, swap(block))]
    blocks += [b for piece in pieces for b in (piece, swap(piece))]

    work = (left_environment_block, right_env)
    cost = pl.CostEstimate(
        flops=4 * tasks * rows * cols * rows, bytes_accessed=4 * tasks * rows * cols, transcendentals=0
    )
    slow = pl.CostEstimate(flops=4 * cost.flops, bytes_accessed=4 * cost.bytes_accessed, transcendentals=0)
    sums = array((sectors, rows, cols), F32)
    acc = call(clear, sums, (), cost=slow)
    scratch = (VMEM((sectors, rows, cols), BF16),)
    streamed = 16 * sums.size > VMEM_BYTES
    if streamed:
        scratch += (VMEM((2, 4, rows, cols), BF16), pltpu.SemaphoreType.DMA((2, 4)))
    operands = (task_in, task_out, *blocks, *work, acc)
    last = len(operands) - 1
    piece = (depth, quarter, cols)
    _, *pieces = call(
        contract,
        (sums, *(array(piece, BF16),) * groups, *(array(piece, F32),) * groups),
        operands,
        scratch,
        scalars=2,
        cost=cost,
        aliases={last: 0},
        streamed=(last - 2, last - 1) if streamed else (),
    )
    sends, keeps = pieces[:groups], pieces[groups:]

    away, here = [], [keeps[0]]
    for j in [*range(1, groups), 0]:
        got = swap(sends[j])
        if j:
            first, last = call(
                merge_cores, (array((depth - 1, *piece[1:]), BF16), array((1, *piece[1:]), BF16)), (keeps[j], got)
            )
            away.append(along_mpo(first, j))
            here.append(along_mpo(last, j))
        else:
            here.append(got)
            away = [keeps[0], got, *away]
    sent = call(functools.partial(merge_away, depth), (array(piece[1:], BF16),) * (depth - 1), away)
    total = call(merge_here, array(piece[1:], F32), here)
    for k, block in enumerate(sent):
        total = total + along_z(block, k + 1, round_z).astype(F32)
    total = total[None]
    return jnp.where(live(total.shape, group * quarter), total, jnp.zeros_like(total)).astype(BF16)


def solution(mesh):
    return jax.shard_map(
        device_step,
        mesh=mesh,
        in_specs=(
            P("sec", None, None),
            P("sec"),
            P("sec"),
            P(("mpo", "sec"), None, None),
            P(("mpo", "sec"), None, None),
            P(("mpo", "sec")),
            P(("mpo", "sec")),
        ),
        out_specs=P("sec", "mpo", None),
        check_vma=False,
    )
```

```python
import functools
import math

import jax
import jax.numpy as jnp
from jax import lax
from jax.experimental import pallas as pl
from jax.experimental.pallas import tpu as pltpu
from jax.sharding import PartitionSpec as P


CORES = 2
UNROLL = 40
DIRECT = (0, 1)
VMEM_BYTES = 67043328
SLACK = 1 << 20
VMEM = pltpu.VMEM
SMEM = pltpu.SMEM
BF16 = jnp.bfloat16
F32 = jnp.float32


def partner(layer, k, depth, back=False):
    if depth & (depth - 1) == 0:
        return layer ^ k
    return lax.rem(layer + (depth - k if back else k), depth) if isinstance(layer, jax.Array) else (layer + k) % depth


def send(value, axis, target):
    return lax.ppermute(value, axis, [(i, target(i)) for i in range(lax.axis_size(axis))])


def along_z(value, k, rule=partner):
    depth = lax.axis_size("sec") // CORES
    return send(value, "sec", lambda i: rule(i // CORES, k, depth) * CORES + i % CORES)


def round_z(layer, k, depth):
    return lax.rem(layer + k, depth) if isinstance(k, jax.Array) else (layer + k) % depth


def far_layer(group, n, groups, depth):
    return len(DIRECT) + group // 2 * (2 * (depth - len(DIRECT)) // groups) + n


def fetch_far(value, n):
    groups, sectors = lax.axis_size("mpo"), lax.axis_size("sec")
    depth = sectors // CORES

    def target(i):
        group, sec = divmod(i, sectors)
        layer = partner(sec // CORES, far_layer(group, n, groups, depth), depth)
        return (group * depth + layer) * CORES + sec % CORES

    return lax.ppermute(value, ("mpo", "sec"), [(i, target(i)) for i in range(groups * sectors)])


def along_mpo(value, j):
    groups = lax.axis_size("mpo")
    return send(value, "mpo", lambda i: (i + j) % groups)


def swap(value):
    return send(value, "sec", lambda i: i ^ 1)


def array(shape, dtype):
    return jax.ShapeDtypeStruct(shape, dtype)


def grant(scratch, *operands):
    mine, others = (sum(math.prod(a.shape) * a.dtype.itemsize for a in group) for group in (scratch, operands))
    return mine + SLACK if 2 * (mine + others) < VMEM_BYTES else min(mine + others + 2 * SLACK, VMEM_BYTES)


def call(kernel, out_shape, operands, scratch=(), scalars=0, cost=None, aliases=None, streamed=()):
    one = not isinstance(out_shape, tuple)
    outs = (out_shape,) if one else out_shape
    specs = [pl.BlockSpec(memory_space=SMEM)] * scalars
    specs += [pl.BlockSpec(memory_space=VMEM)] * (len(operands) - scalars)
    for n in streamed:
        specs[n] = pl.BlockSpec(memory_space=pl.ANY)
    run = pl.pallas_call(
        kernel,
        out_shape=outs,
        in_specs=specs,
        out_specs=(pl.BlockSpec(memory_space=VMEM),) * len(outs),
        scratch_shapes=scratch,
        cost_estimate=cost,
        input_output_aliases=aliases or {},
        compiler_params=pltpu.CompilerParams(
            vmem_limit_bytes=grant(
                [s for s in scratch if getattr(s, "memory_space", None) == VMEM], *outs, *operands[scalars:]
            )
        ),
    )
    results = run(*operands)
    return results[0] if one else results


def clear(acc):
    acc[...] = jnp.zeros_like(acc)


def take_rows(own, part):
    half = part.shape[1]
    start = lax.rem(lax.axis_index("mpo"), 2) * half
    part[...] = own[:, pl.ds(pl.multiple_of(start, half), half)]


def products(ids, blocks, left, right, acc, *stage):
    tasks = left.shape[0]
    limit = stage[0].shape[1] if stage else UNROLL
    unroll = max(n for n in range(1, limit + 1) if tasks % n == 0)

    def fetch(which, t, u):
        source = (left, right)[which]
        if not stage:
            return source[t]
        target, sems = stage
        copy = pltpu.make_async_copy(source.at[t], target.at[which, u], sems.at[which, u])
        copy.start()
        copy.wait()
        return target[which, u]

    lanes = lax.broadcasted_iota(jnp.int32, ids.shape, 1)
    sectors = blocks.shape[0]

    def step(n, _):
        for u in range(unroll):
            t = n * unroll + u
            code = jnp.max(jnp.where(lanes == t, ids[...], 0.0)).astype(jnp.int32)
            source, target = lax.div(code, sectors), lax.rem(code, sectors)
            middle = jnp.dot(fetch(0, t, u), blocks[source], preferred_element_type=F32).astype(BF16)
            acc[target] += lax.dot_general(
                middle, fetch(1, t, u), (((1,), (1,)), ((), ())), preferred_element_type=F32
            )
        return 0

    lax.fori_loop(0, tasks // unroll, step, 0)


def contract(ids, *refs):
    groups = lax.axis_size("mpo")
    direct, refs = refs[: CORES * len(DIRECT)], refs[CORES * len(DIRECT) :]
    spread, (left, right, _, acc), refs = refs[: CORES * groups], refs[CORES * groups :][:4], refs[CORES * groups + 4 :]
    sends, keeps, (blocks, *stage) = refs[:groups], refs[groups : 2 * groups], refs[2 * groups :]
    depth, quarter = sends[0].shape[:2]
    sec = lax.axis_index("sec")
    layer, core = sec // CORES, sec % CORES
    group = lax.axis_index("mpo")
    for n, k in enumerate(DIRECT):
        base = partner(layer, k, depth, back=True) * CORES
        blocks[base + core] = direct[CORES * n][0]
        blocks[base + 1 - core] = direct[CORES * n + 1][0]
    rounds, half = spread[0].shape[:2]
    for j in range(groups):
        source = lax.rem(group + groups - j, groups)
        rows = pl.ds(pl.multiple_of(lax.rem(source, 2) * half, half), half)
        for n in range(rounds):
            k = len(DIRECT) + lax.div(source, 2) * rounds + n
            base = partner(layer, k, depth, back=True) * CORES
            blocks[base + core, rows] = spread[CORES * j][n]
            blocks[base + 1 - core, rows] = spread[CORES * j + 1][n]
    products(ids, blocks, left, right, acc, *stage)

    def put(k, _):
        base = round_z(layer, k, depth) * CORES
        for j in range(groups):
            rows = pl.ds(pl.multiple_of(lax.rem(group + j, groups) * quarter, quarter), quarter)
            keeps[j][k] = acc[base + core, rows]
            sends[j][k] = acc[base + 1 - core, rows].astype(BF16)
        return 0

    lax.fori_loop(0, depth, put, 0)


def merge_cores(keep, got, away, here):
    value = keep[...] + got[...].astype(F32)
    here[...] = value[:1].astype(BF16)
    away[...] = value[1:].astype(BF16)


def merge_away(depth, *refs):
    terms, sends = refs[: 1 - depth], refs[1 - depth :]
    for k in range(1, depth):
        values = [term[k + term.shape[0] - depth].astype(F32) for term in terms]
        sends[k - 1][...] = functools.reduce(jnp.add, values).astype(BF16)


def merge_here(*refs):
    *terms, total = refs
    total[...] = functools.reduce(jnp.add, [term[0].astype(F32) for term in terms])


def device_step(
    wavefunction, left_dims, right_dims, left_environment_block, right_env, task_out, task_in
):
    rows, cols = wavefunction.shape[1:]
    groups = lax.axis_size("mpo")
    sectors = lax.axis_size("sec")
    depth = sectors // CORES
    quarter = rows // groups
    tasks = task_out.shape[0]
    group = lax.axis_index("mpo")

    def live(shape, first_row):
        row_ids = lax.broadcasted_iota(jnp.int32, shape, 1) + first_row
        col_ids = lax.broadcasted_iota(jnp.int32, shape, 2)
        return (row_ids < left_dims[:, None, None]) & (col_ids < right_dims[:, None, None])

    own = jnp.where(live(wavefunction.shape, 0), wavefunction, jnp.zeros_like(wavefunction))
    part = call(take_rows, array((1, rows // 2, cols), BF16), (own,))
    assert groups % 2 == 0 and 2 * (depth - len(DIRECT)) % groups == 0
    rounds = 2 * (depth - len(DIRECT)) // groups
    far = [fetch_far(part, n) for n in range(rounds)]
    near = [own, *(along_z(own, k) for k in DIRECT[1:])]
    pieces = [jnp.concatenate(far, axis=0) if rounds > 1 else far[0]]
    pieces += [along_mpo(pieces[0], j) for j in range(1, groups)]
    blocks = [b for block in near for b in (block, swap(block))]
    blocks += [b for piece in pieces for b in (piece, swap(piece))]

    work = (left_environment_block, right_env)
    cost = pl.CostEstimate(
        flops=4 * tasks * rows * cols * rows, bytes_accessed=4 * tasks * rows * cols, transcendentals=0
    )
    slow = pl.CostEstimate(flops=4 * cost.flops, bytes_accessed=4 * cost.bytes_accessed, transcendentals=0)
    sums = array((sectors, rows, cols), F32)
    acc = call(clear, sums, (), cost=slow)
    scratch = (VMEM((sectors, rows, cols), BF16),)
    streamed = 16 * sums.size > VMEM_BYTES
    if streamed:
        scratch += (VMEM((2, 4, rows, cols), BF16), pltpu.SemaphoreType.DMA((2, 4)))
    ids = (task_in * sectors + task_out).astype(F32)[None]
    operands = (ids, *blocks, *work, acc)
    last = len(operands) - 1
    piece = (depth, quarter, cols)
    _, *pieces = call(
        contract,
        (sums, *(array(piece, BF16),) * groups, *(array(piece, F32),) * groups),
        operands,
        scratch,
        cost=cost,
        aliases={last: 0},
        streamed=(last - 2, last - 1) if streamed else (),
    )
    sends, keeps = pieces[:groups], pieces[groups:]

    away, here = [], [keeps[0]]
    for j in [*range(1, groups), 0]:
        got = swap(sends[j])
        if j:
            first, last = call(
                merge_cores, (array((depth - 1, *piece[1:]), BF16), array((1, *piece[1:]), BF16)), (keeps[j], got)
            )
            away.append(along_mpo(first, j))
            here.append(along_mpo(last, j))
        else:
            here.append(got)
            away = [keeps[0], got, *away]
    sent = call(functools.partial(merge_away, depth), (array(piece[1:], BF16),) * (depth - 1), away)
    total = call(merge_here, array(piece[1:], F32), here)
    for k, block in enumerate(sent):
        total = total + along_z(block, k + 1, round_z).astype(F32)
    total = total[None]
    return jnp.where(live(total.shape, group * quarter), total, jnp.zeros_like(total)).astype(BF16)


def solution(mesh):
    return jax.shard_map(
        device_step,
        mesh=mesh,
        in_specs=(
            P("sec", None, None),
            P("sec"),
            P("sec"),
            P(("mpo", "sec"), None, None),
            P(("mpo", "sec"), None, None),
            P(("mpo", "sec")),
            P(("mpo", "sec")),
        ),
        out_specs=P("sec", "mpo", None),
        check_vma=False,
    )
```

```python
import functools
import math

import jax
import jax.numpy as jnp
from jax import lax
from jax.experimental import pallas as pl
from jax.experimental.pallas import tpu as pltpu
from jax.sharding import PartitionSpec as P


CORES = 2
UNROLL = 40
DIRECT = (0, 1)
VMEM_BYTES = 67043328
SLACK = 1 << 20
VMEM = pltpu.VMEM
SMEM = pltpu.SMEM
BF16 = jnp.bfloat16
F32 = jnp.float32


def partner(layer, k, depth, back=False):
    if depth & (depth - 1) == 0:
        return layer ^ k
    return lax.rem(layer + (depth - k if back else k), depth) if isinstance(layer, jax.Array) else (layer + k) % depth


def send(value, axis, target):
    return lax.ppermute(value, axis, [(i, target(i)) for i in range(lax.axis_size(axis))])


def along_z(value, k, rule=partner):
    depth = lax.axis_size("sec") // CORES
    return send(value, "sec", lambda i: rule(i // CORES, k, depth) * CORES + i % CORES)


def round_z(layer, k, depth):
    return lax.rem(layer + k, depth) if isinstance(k, jax.Array) else (layer + k) % depth


def far_layer(group, n, groups, depth):
    return len(DIRECT) + group // 2 * (2 * (depth - len(DIRECT)) // groups) + n


def fetch_far(value, n):
    groups, sectors = lax.axis_size("mpo"), lax.axis_size("sec")
    depth = sectors // CORES

    def target(i):
        group, sec = divmod(i, sectors)
        layer = partner(sec // CORES, far_layer(group, n, groups, depth), depth)
        return (group * depth + layer) * CORES + sec % CORES

    return lax.ppermute(value, ("mpo", "sec"), [(i, target(i)) for i in range(groups * sectors)])


def along_mpo(value, j):
    groups = lax.axis_size("mpo")
    return send(value, "mpo", lambda i: (i + j) % groups)


def swap(value):
    return send(value, "sec", lambda i: i ^ 1)


def array(shape, dtype):
    return jax.ShapeDtypeStruct(shape, dtype)


def grant(scratch, *operands):
    mine, others = (sum(math.prod(a.shape) * a.dtype.itemsize for a in group) for group in (scratch, operands))
    return mine + SLACK if 2 * (mine + others) < VMEM_BYTES else min(mine + others + 2 * SLACK, VMEM_BYTES)


def call(kernel, out_shape, operands, scratch=(), scalars=0, cost=None, aliases=None, streamed=()):
    one = not isinstance(out_shape, tuple)
    outs = (out_shape,) if one else out_shape
    specs = [pl.BlockSpec(memory_space=SMEM)] * scalars
    specs += [pl.BlockSpec(memory_space=VMEM)] * (len(operands) - scalars)
    for n in streamed:
        specs[n] = pl.BlockSpec(memory_space=pl.ANY)
    run = pl.pallas_call(
        kernel,
        out_shape=outs,
        in_specs=specs,
        out_specs=(pl.BlockSpec(memory_space=VMEM),) * len(outs),
        scratch_shapes=scratch,
        cost_estimate=cost,
        input_output_aliases=aliases or {},
        compiler_params=pltpu.CompilerParams(
            vmem_limit_bytes=grant(
                [s for s in scratch if getattr(s, "memory_space", None) == VMEM], *outs, *operands[scalars:]
            )
        ),
    )
    results = run(*operands)
    return results[0] if one else results


def clear(acc):
    acc[...] = jnp.zeros_like(acc)


def products(ids, blocks, left, right, acc, *stage):
    tasks = left.shape[0]
    limit = stage[0].shape[1] if stage else UNROLL
    unroll = max(n for n in range(1, limit + 1) if tasks % n == 0)

    def fetch(which, t, u):
        source = (left, right)[which]
        if not stage:
            return source[t]
        target, sems = stage
        copy = pltpu.make_async_copy(source.at[t], target.at[which, u], sems.at[which, u])
        copy.start()
        copy.wait()
        return target[which, u]

    lanes = lax.broadcasted_iota(jnp.int32, ids.shape, 1)
    sectors = blocks.shape[0]

    def step(n, _):
        for u in range(unroll):
            t = n * unroll + u
            code = jnp.max(jnp.where(lanes == t, ids[...], 0.0)).astype(jnp.int32)
            source, target = lax.div(code, sectors), lax.rem(code, sectors)
            middle = jnp.dot(fetch(0, t, u), blocks[source], preferred_element_type=F32).astype(BF16)
            acc[target] += lax.dot_general(
                middle, fetch(1, t, u), (((1,), (1,)), ((), ())), preferred_element_type=F32
            )
        return 0

    lax.fori_loop(0, tasks // unroll, step, 0)


def contract(ids, *refs):
    groups = lax.axis_size("mpo")
    direct, refs = refs[: CORES * len(DIRECT)], refs[CORES * len(DIRECT) :]
    spread, (left, right, _, acc), refs = refs[: CORES * groups], refs[CORES * groups :][:4], refs[CORES * groups + 4 :]
    sends, keeps, (blocks, *stage) = refs[:groups], refs[groups : 2 * groups], refs[2 * groups :]
    depth, quarter = sends[0].shape[:2]
    sec = lax.axis_index("sec")
    layer, core = sec // CORES, sec % CORES
    group = lax.axis_index("mpo")
    for n, k in enumerate(DIRECT):
        base = partner(layer, k, depth, back=True) * CORES
        blocks[base + core] = direct[CORES * n][0]
        blocks[base + 1 - core] = direct[CORES * n + 1][0]
    rounds, half = spread[0].shape[:2]
    for j in range(groups):
        source = lax.rem(group + groups - j, groups)
        rows = pl.ds(pl.multiple_of(lax.rem(source, 2) * half, half), half)
        for n in range(rounds):
            k = len(DIRECT) + lax.div(source, 2) * rounds + n
            base = partner(layer, k, depth, back=True) * CORES
            blocks[base + core, rows] = spread[CORES * j][n]
            blocks[base + 1 - core, rows] = spread[CORES * j + 1][n]
    products(ids, blocks, left, right, acc, *stage)

    def put(k, _):
        base = round_z(layer, k, depth) * CORES
        for j in range(groups):
            rows = pl.ds(pl.multiple_of(lax.rem(group + j, groups) * quarter, quarter), quarter)
            keeps[j][k] = acc[base + core, rows]
            sends[j][k] = acc[base + 1 - core, rows].astype(BF16)
        return 0

    lax.fori_loop(0, depth, put, 0)


def merge_cores(keep, got, away, here):
    value = keep[...] + got[...].astype(F32)
    here[...] = value[:1].astype(BF16)
    away[...] = value[1:].astype(BF16)


def merge_away(depth, *refs):
    terms, sends = refs[: 1 - depth], refs[1 - depth :]
    for k in range(1, depth):
        values = [term[k + term.shape[0] - depth].astype(F32) for term in terms]
        sends[k - 1][...] = functools.reduce(jnp.add, values).astype(BF16)


def merge_here(*refs):
    *terms, total = refs
    total[...] = functools.reduce(jnp.add, [term[0].astype(F32) for term in terms])


def device_step(
    wavefunction, left_dims, right_dims, left_environment_block, right_env, task_out, task_in
):
    rows, cols = wavefunction.shape[1:]
    groups = lax.axis_size("mpo")
    sectors = lax.axis_size("sec")
    depth = sectors // CORES
    quarter = rows // groups
    tasks = task_out.shape[0]
    group = lax.axis_index("mpo")

    def live(shape, first_row):
        row_ids = lax.broadcasted_iota(jnp.int32, shape, 1) + first_row
        col_ids = lax.broadcasted_iota(jnp.int32, shape, 2)
        return (row_ids < left_dims[:, None, None]) & (col_ids < right_dims[:, None, None])

    own = jnp.where(live(wavefunction.shape, 0), wavefunction, jnp.zeros_like(wavefunction))
    half = rows // 2
    start = lax.rem(group, 2) * half
    part = lax.dynamic_slice_in_dim(wavefunction, start, half, axis=1)
    part = jnp.where(live(part.shape, start), part, jnp.zeros_like(part))
    assert groups % 2 == 0 and 2 * (depth - len(DIRECT)) % groups == 0
    rounds = 2 * (depth - len(DIRECT)) // groups
    far = [fetch_far(part, n) for n in range(rounds)]
    near = [own, *(along_z(own, k) for k in DIRECT[1:])]
    pieces = [jnp.concatenate(far, axis=0) if rounds > 1 else far[0]]
    pieces += [along_mpo(pieces[0], j) for j in range(1, groups)]
    blocks = [b for block in near for b in (block, swap(block))]
    blocks += [b for piece in pieces for b in (piece, swap(piece))]

    work = (left_environment_block, right_env)
    cost = pl.CostEstimate(
        flops=4 * tasks * rows * cols * rows, bytes_accessed=4 * tasks * rows * cols, transcendentals=0
    )
    slow = pl.CostEstimate(flops=4 * cost.flops, bytes_accessed=4 * cost.bytes_accessed, transcendentals=0)
    sums = array((sectors, rows, cols), F32)
    acc = call(clear, sums, (), cost=slow)
    scratch = (VMEM((sectors, rows, cols), BF16),)
    streamed = 16 * sums.size > VMEM_BYTES
    if streamed:
        scratch += (VMEM((2, 4, rows, cols), BF16), pltpu.SemaphoreType.DMA((2, 4)))
    ids = (task_in * sectors + task_out).astype(F32)[None]
    operands = (ids, *blocks, *work, acc)
    last = len(operands) - 1
    piece = (depth, quarter, cols)
    _, *pieces = call(
        contract,
        (sums, *(array(piece, BF16),) * groups, *(array(piece, F32),) * groups),
        operands,
        scratch,
        cost=cost,
        aliases={last: 0},
        streamed=(last - 2, last - 1) if streamed else (),
    )
    sends, keeps = pieces[:groups], pieces[groups:]

    away, here = [], [keeps[0]]
    for j in [*range(1, groups), 0]:
        got = swap(sends[j])
        if j:
            first, last = call(
                merge_cores, (array((depth - 1, *piece[1:]), BF16), array((1, *piece[1:]), BF16)), (keeps[j], got)
            )
            away.append(along_mpo(first, j))
            here.append(along_mpo(last, j))
        else:
            here.append(got)
            away = [keeps[0], got, *away]
    sent = call(functools.partial(merge_away, depth), (array(piece[1:], BF16),) * (depth - 1), away)
    total = call(merge_here, array(piece[1:], F32), here)
    for k, block in enumerate(sent):
        total = total + along_z(block, k + 1, round_z).astype(F32)
    total = total[None]
    return jnp.where(live(total.shape, group * quarter), total, jnp.zeros_like(total)).astype(BF16)


def solution(mesh):
    return jax.shard_map(
        device_step,
        mesh=mesh,
        in_specs=(
            P("sec", None, None),
            P("sec"),
            P("sec"),
            P(("mpo", "sec"), None, None),
            P(("mpo", "sec"), None, None),
            P(("mpo", "sec")),
            P(("mpo", "sec")),
        ),
        out_specs=P("sec", "mpo", None),
        check_vma=False,
    )
```
